32 devices in a mesh: rep: 8 (over z, core), tp: 4 (over y, x).
Axes of the slice: x: 2, y: 2, z: 4, core: 2. Of those that a mesh axis runs over, the one named last changes fastest.
Arguments:
- hidden_state: bfloat16 [32, 3584], P('rep'), may hold values from -6 to 6
- lengths: int32 [32], P('rep'), may hold values from 1 to 2048, as said below
- old_qkv: bfloat16 [3584, 4608], P(None, 'tp'), may hold values from -0.09375 to 0.09375
- old_out: bfloat16 [3584, 3584], P(None, 'tp'), may hold values from -0.09375 to 0.09375
- cache_keys: bfloat16 [32, 2048, 512], P('rep', 'tp'), may hold values from -64 to 64
- cache_values: bfloat16 [32, 2048, 512], P('rep', 'tp'), may hold values from -6 to 6
- new_qkv: bfloat16 [3584, 4608], P(('rep', 'tp')), may hold values from -0.09375 to 0.09375
- new_out: bfloat16 [3584, 3584], P(('rep', 'tp')), may hold values from -0.09375 to 0.09375
Outputs:
- decoded: bfloat16 [32, 3584], P('rep', 'tp')
- resharded_qkv: bfloat16 [3584, 4608], P(None, 'tp')
- resharded_out: bfloat16 [3584, 3584], P(None, 'tp')
The draws below stay inside these ranges and needn't reach their ends.
Inputs may be any that keep to these rules, and one draw needn't show every extreme that they name: Every sequence has 1 to 2048 cached tokens, held in positions 0 to lengths - 1; in every draw some sequence fills its cache.
All inputs are finite; a program needn't handle non-finite values.
Results may differ from the reference program's by a relative error of at most 0.012.
Values may be sent and summed in bfloat16 or wider, within the bound.
A program may use at most 128 MiB of HBM per device.

```python
import jax
import jax.numpy as jnp
from jax import lax

D = 3584
HQ = 28
KVH = 4
HD = 128
SEQS = 32
CACHE_LEN = 2048
COLS = 4608


def draw_lengths(key, part):
    drawn = jax.random.randint(key, (SEQS,), 1, CACHE_LEN + 1)
    chosen = jax.random.randint(jax.random.fold_in(key, 7), (), 0, SEQS)
    return jnp.where(jnp.arange(SEQS) == chosen, CACHE_LEN, drawn).astype(jnp.int32)


def draw_cache_keys(key, part):
    drawn = jax.random.normal(key, (SEQS, CACHE_LEN, KVH * HD), jnp.float32)
    return jnp.clip(drawn, -64.0, 64.0).astype(jnp.bfloat16)


def levels(rng, dims, pieces, least, largest):
    level = 1.0
    for axis_at, shards_of in pieces:
        steps = jax.random.uniform(jax.random.fold_in(jax.random.fold_in(rng, 6), axis_at), (shards_of,), jnp.float32, least / len(pieces), largest / len(pieces))
        level = level * jnp.repeat(jnp.exp(steps), dims[axis_at] // shards_of).reshape((-1,) + (1,) * (len(dims) - 1 - axis_at))
    return level


def bell_draw(stream_key, shape, deviation, bound, cuts=(), kind=jnp.bfloat16):
    values = deviation * jax.random.normal(stream_key, shape, jnp.float32)
    if cuts:
        values = values * levels(stream_key, shape, cuts, -0.22, 0.18)
    return jnp.clip(values, -bound, bound).astype(kind)


def setup_inputs(seed: int = 0) -> dict:
    splits = jax.random.split(jax.random.key(seed), 9)
    return {
        "hidden_state": bell_draw(splits[0], (SEQS, D), 1.0, 6.0, ((0, 8),)),
        "lengths": draw_lengths(jax.random.fold_in(splits[8], 71), 0),
        "old_qkv": bell_draw(splits[2], (D, COLS), D ** -0.5, 0.09375, ((1, 4),)),
        "old_out": bell_draw(splits[3], (HQ * HD, D), (HQ * HD) ** -0.5, 0.09375, ((1, 4),)),
        "cache_keys": draw_cache_keys(jax.random.fold_in(splits[8], 71), 0),
        "cache_values": bell_draw(splits[5], (SEQS, CACHE_LEN, KVH * HD), 1.0, 6.0, ((0, 8), (1, 4))),
        "new_qkv": bell_draw(splits[6], (D, COLS), D ** -0.5, 0.09375, ((0, 32),)),
        "new_out": bell_draw(splits[7], (HQ * HD, D), (HQ * HD) ** -0.5, 0.09375, ((0, 32),)),
    }


ROPE_BASE = 1000000.0

def rotate(vectors, positions):
    half_dim = vectors.shape[-1] // 2
    frequency = ROPE_BASE ** (-2.0 * jnp.arange(half_dim, dtype=jnp.float32) / (2 * half_dim))
    angles = positions.astype(jnp.float32)[:, None, None] * frequency
    first_half = vectors[..., :half_dim]
    second_half = vectors[..., half_dim:]
    return jnp.concatenate([first_half * jnp.cos(angles) - second_half * jnp.sin(angles), second_half * jnp.cos(angles) + first_half * jnp.sin(angles)], axis=-1)

def reference(hidden_state, lengths, old_qkv, old_out, cache_keys, cache_values, new_qkv, new_out):
    joined = jnp.dot(hidden_state, old_qkv, preferred_element_type=jnp.float32).astype(jnp.bfloat16)
    q_width = HQ * HD
    k_width = KVH * HD
    queries = rotate(joined[:, :q_width].astype(jnp.float32).reshape(SEQS, HQ, HD), lengths).astype(jnp.bfloat16)
    own_keys = rotate(joined[:, q_width:q_width + k_width].astype(jnp.float32).reshape(SEQS, KVH, HD), lengths).astype(jnp.bfloat16)
    own_values = joined[:, q_width + k_width:].reshape(SEQS, KVH, HD)
    group_size = HQ // KVH
    inv_root = 1.0 / jnp.sqrt(jnp.float32(HD))

    def attend(per_sequence):
        query_row, own_key, own_value, length, seq_keys, seq_values = per_sequence
        grouped = query_row.reshape(KVH, group_size, HD).astype(jnp.float32)
        key_blocks = seq_keys.reshape(CACHE_LEN, KVH, HD).astype(jnp.float32)
        value_blocks = seq_values.reshape(CACHE_LEN, KVH, HD).astype(jnp.float32)
        scores = jnp.einsum('kgd,tkd->kgt', grouped, key_blocks) * inv_root
        live_mask = jnp.arange(CACHE_LEN, dtype=jnp.int32) < length
        scores = jnp.where(live_mask, scores, jnp.float32(-1e+30))
        own_score = lax.optimization_barrier(jnp.sum(grouped * own_key.astype(jnp.float32)[:, None, :], axis=-1)) * inv_root
        top_score = jnp.maximum(lax.optimization_barrier(jnp.max(scores, axis=-1)), own_score)
        weights = jnp.where(live_mask, jnp.exp(scores - top_score[..., None]), jnp.float32(0.0)).astype(jnp.bfloat16)
        own_weight = lax.optimization_barrier(jnp.exp(own_score - top_score).astype(jnp.bfloat16)).astype(jnp.float32)
        numerator = jnp.einsum('kgt,tkd->kgd', weights.astype(jnp.float32), value_blocks)
        numerator = numerator + own_weight[..., None] * own_value.astype(jnp.float32)[:, None, :]
        denominator = lax.optimization_barrier(jnp.sum(weights.astype(jnp.float32), axis=-1)) + own_weight
        return (numerator / denominator[..., None]).reshape(HQ * HD).astype(jnp.bfloat16)
    attended = lax.map(attend, (queries, own_keys, own_values, lengths, cache_keys, cache_values))
    decoded = jnp.dot(attended, old_out, preferred_element_type=jnp.float32).astype(jnp.bfloat16)
    return (decoded, new_qkv, new_out)
```

```python
import functools

import jax
import jax.numpy as jnp
from jax import lax
from jax.experimental import pallas as pl
from jax.experimental.pallas import tpu as pltpu
from jax.sharding import PartitionSpec as P

HQ = 28
KVH = 4
HD = 128


ROPE_BASE = 1000000.0


def rotate(vectors, positions):
    half_dim = vectors.shape[-1] // 2
    frequency = ROPE_BASE ** (-2.0 * jnp.arange(half_dim, dtype=jnp.float32) / (2 * half_dim))
    angles = positions.astype(jnp.float32)[:, None, None] * frequency
    first_half = vectors[..., :half_dim]
    second_half = vectors[..., half_dim:]
    return jnp.concatenate(
        [
            first_half * jnp.cos(angles) - second_half * jnp.sin(angles),
            second_half * jnp.cos(angles) + first_half * jnp.sin(angles),
        ],
        axis=-1,
    )


def per_device(hidden_state, lengths, old_qkv, old_out, cache_keys, cache_values):
    seq_count = hidden_state.shape[0]
    local_joined = jnp.dot(hidden_state, old_qkv, preferred_element_type=jnp.float32).astype(
        jnp.bfloat16
    )
    joined_rows = lax.all_gather(local_joined, "tp", axis=1, tiled=True)
    q_width = HQ * HD
    k_width = KVH * HD
    group_size = HQ // KVH
    queries = rotate(
        joined_rows[:, :q_width].astype(jnp.float32).reshape(seq_count, HQ, HD), lengths
    ).astype(jnp.bfloat16)
    own_keys = rotate(
        joined_rows[:, q_width : q_width + k_width].astype(jnp.float32).reshape(seq_count, KVH, HD),
        lengths,
    ).astype(jnp.bfloat16)
    own_values = joined_rows[:, q_width + k_width :].reshape(seq_count, KVH, HD)
    inv_root = 1.0 / jnp.sqrt(jnp.float32(HD))
    cache_rows = cache_keys.shape[1]
    grouped = queries.reshape(seq_count, KVH, group_size, HD)
    key_blocks = cache_keys.reshape(seq_count, cache_rows, KVH, HD)
    value_blocks = cache_values.reshape(seq_count, cache_rows, KVH, HD)
    scores = (
        jnp.einsum("skgd,stkd->skgt", grouped, key_blocks, preferred_element_type=jnp.float32)
        * inv_root
    )
    positions = lax.axis_index("tp") * cache_rows + jnp.arange(cache_rows, dtype=jnp.int32)
    live_mask = (positions[None, :] < lengths[:, None])[:, None, None, :]
    scores = jnp.where(live_mask, scores, jnp.float32(-1e30))
    own_score = (
        jnp.sum(grouped.astype(jnp.float32) * own_keys.astype(jnp.float32)[:, :, None, :], axis=-1)
        * inv_root
    )
    local_top = jnp.maximum(jnp.max(scores, axis=-1), own_score)
    top_score = lax.pmax(local_top, "tp")
    weights = jnp.where(live_mask, jnp.exp(scores - top_score[..., None]), jnp.float32(0.0)).astype(
        jnp.bfloat16
    )
    numer_part = jnp.einsum(
        "skgt,stkd->skgd", weights, value_blocks, preferred_element_type=jnp.float32
    )
    denom_part = jnp.sum(weights.astype(jnp.float32), axis=-1)
    numerator, denominator = lax.psum((numer_part, denom_part), "tp")
    own_weight = lax.optimization_barrier(
        jnp.exp(own_score - top_score).astype(jnp.bfloat16)
    ).astype(jnp.float32)
    numerator = numerator + own_weight[..., None] * own_values.astype(jnp.float32)[:, :, None, :]
    denominator = denominator + own_weight
    attended = (numerator / denominator[..., None]).reshape(seq_count, q_width).astype(jnp.bfloat16)
    decoded = jnp.dot(attended, old_out, preferred_element_type=jnp.float32).astype(jnp.bfloat16)
    return decoded


def native_move(new_qkv, new_out):
    def move(block):
        piece = lax.all_to_all(block, "tp", split_axis=1, concat_axis=0, tiled=True)
        return lax.all_gather(piece, "rep", axis=0, tiled=True)

    return move(new_qkv), move(new_out)


def flip(index, bits, size):
    out = index
    bit = 1
    while bit < size:
        if (bits // bit) % 2:
            out = out + bit - 2 * bit * ((index // bit) % 2)
        bit *= 2
    return out


def move_kernel(reps, tps, qkv_ref, out_ref, qkv_full, out_full, *sems):
    (a_send, a_recv, p_send, p_recv, m_send, m_recv, s_send, s_recv, own_sem) = sems
    planes = reps // 2
    rep, tp = lax.axis_index("rep"), lax.axis_index("tp")
    plane, core = rep // 2, rep % 2
    rows = qkv_ref.shape[0]
    blocks, fulls = (qkv_ref, out_ref), (qkv_full, out_full)
    widths = (qkv_full.shape[1], out_full.shape[1])
    up = (lax.rem(plane + 1, planes) * 2 + core, tp)
    down = (lax.rem(plane + planes - 1, planes) * 2 + core, tp)
    twin = (plane * 2 + 1 - core, tp)
    peers = [(rep, flip(tp, k, tps)) for k in range(1, tps)]

    barrier = pltpu.get_barrier_semaphore()
    partners = [up, down, twin] + peers
    for device in partners:
        pl.semaphore_signal(barrier, inc=1, device_id=device, device_id_type=pl.DeviceIdType.MESH)
    pl.semaphore_wait(barrier, len(partners))

    def rows_of(distance, k, w):
        source = lax.rem(plane + planes - distance, planes) * 2 + core
        start = (source * tps + flip(tp, k, tps)) * rows
        return fulls[w].at[pl.ds(pl.multiple_of(start, rows), rows)]

    def column(w, t):
        start = pl.multiple_of(t * widths[w], 128)
        return blocks[w].at[:, pl.ds(start, widths[w])]

    def remote(source, target, send, recv, device):
        copy = pltpu.make_async_remote_copy(
            src_ref=source, dst_ref=target, send_sem=send, recv_sem=recv,
            device_id=device, device_id_type=pl.DeviceIdType.MESH,
        )
        return copy

    sent = []

    def spread(distance, k, w, above, below, source=None):
        target = rows_of(distance, k, w)
        source = target if source is None else source
        if above:
            hop = distance % planes
            copy = remote(source, target, p_send.at[hop, k, w], p_recv.at[hop, k, w], up)
            copy.start()
            sent.append(copy)
        if below:
            hop = (planes - distance) % planes
            copy = remote(source, target, m_send.at[hop, k, w], m_recv.at[hop, k, w], down)
            copy.start()
            sent.append(copy)
        copy = remote(source, target, s_send.at[distance, k, w], s_recv.at[distance, k, w], twin)
        copy.start()
        sent.append(copy)

    def arrived_up(hop, k, w):
        target = rows_of(hop + 1, k, w)
        remote(target, target, p_send.at[hop, k, w], p_recv.at[hop, k, w], up).wait_recv()

    def arrived_down(hop, k, w):
        target = rows_of(planes - hop - 1, k, w)
        remote(target, target, m_send.at[hop, k, w], m_recv.at[hop, k, w], down).wait_recv()

    local = []
    for k in range(1, tps):
        for w in range(2):
            copy = remote(
                column(w, flip(tp, k, tps)), rows_of(0, 0, w),
                a_send.at[k, w], a_recv.at[k, w], peers[k - 1],
            )
            copy.start()
            sent.append(copy)
    for w in range(2):
        spread(0, 0, w, True, True, column(w, tp))
        copy = pltpu.make_async_copy(column(w, tp), rows_of(0, 0, w), own_sem.at[w])
        copy.start()
        local.append(copy)
    for k in range(1, tps):
        for w in range(2):
            target = rows_of(0, k, w)
            remote(target, target, a_send.at[k, w], a_recv.at[k, w], peers[k - 1]).wait_recv()
            spread(0, k, w, True, True)

    half = planes // 2
    for distance in range(1, half):
        for k in range(tps):
            for w in range(2):
                last = distance + 1 == half
                arrived_up(distance - 1, k, w)
                spread(distance, k, w, not last or k < tps // 2, False)
                arrived_down(distance - 1, k, w)
                spread(planes - distance, k, w, False, not last or k >= tps // 2)
    for k in range(tps // 2):
        for w in range(2):
            arrived_up(half - 1, k, w)
            spread(half, k, w, False, False)
            other = k + tps // 2
            arrived_down(half - 1, other, w)
            spread(half, other, w, False, False)

    for distance in range(planes):
        for k in range(tps):
            for w in range(2):
                source = lax.rem(plane + planes - distance, planes) * 2 + 1 - core
                start = (source * tps + flip(tp, k, tps)) * rows
                target = fulls[w].at[pl.ds(pl.multiple_of(start, rows), rows)]
                remote(
                    target, target, s_send.at[distance, k, w], s_recv.at[distance, k, w], twin
                ).wait_recv()
    for copy in sent:
        copy.wait_send()
    for copy in local:
        copy.wait()


def move(mesh, new_qkv, new_out):
    reps, tps = mesh.shape["rep"], mesh.shape["tp"]
    rows = new_qkv.shape[0]
    widths = (new_qkv.shape[1] // tps, new_out.shape[1] // tps)
    tiled = rows % 16 == 0 and all(width % 128 == 0 for width in widths)
    if reps % 4 or not tiled:
        return native_move(new_qkv, new_out)
    planes = reps // 2
    sem = pltpu.SemaphoreType.DMA
    return pl.pallas_call(
        functools.partial(move_kernel, reps, tps),
        out_shape=[
            jax.ShapeDtypeStruct((rows * reps * tps, width), new_qkv.dtype) for width in widths
        ],
        in_specs=[pl.BlockSpec(memory_space=pl.ANY)] * 2,
        out_specs=[pl.BlockSpec(memory_space=pl.ANY)] * 2,
        scratch_shapes=[sem((tps, 2)), sem((tps, 2))]
        + [sem((planes // 2, tps, 2)) for _ in range(4)]
        + [sem((planes, tps, 2)), sem((planes, tps, 2)), sem((2,))],
        compiler_params=pltpu.CompilerParams(collective_id=0, has_side_effects=True),
    )(new_qkv, new_out)


def solution(mesh):
    in_specs = (
        P("rep", None),
        P("rep"),
        P(None, "tp"),
        P(None, "tp"),
        P("rep", "tp", None),
        P("rep", "tp", None),
        P(("rep", "tp"), None),
        P(("rep", "tp"), None),
    )
    out_specs = (P("rep", "tp"), P(None, "tp"), P(None, "tp"))

    def step(*args):
        decoded = per_device(*args[:6])
        return (decoded, *move(mesh, *args[6:]))

    return jax.shard_map(
        step, mesh=mesh, in_specs=in_specs, out_specs=out_specs, check_vma=False
    )
```

```python
import functools

import jax
import jax.numpy as jnp
from jax import lax
from jax.experimental import pallas as pl
from jax.experimental.pallas import tpu as pltpu
from jax.sharding import PartitionSpec as P

HQ = 28
KVH = 4
HD = 128
PAD = 8
VMEM_BYTES = 67043328
SLACK = 600000
MESH = pl.DeviceIdType.MESH


ROPE_BASE = 1000000.0


def rotate(vectors, positions):
    half_dim = vectors.shape[-1] // 2
    frequency = ROPE_BASE ** (-2.0 * jnp.arange(half_dim, dtype=jnp.float32) / (2 * half_dim))
    angles = positions.astype(jnp.float32)[:, None, None] * frequency
    first_half = vectors[..., :half_dim]
    second_half = vectors[..., half_dim:]
    return jnp.concatenate(
        [
            first_half * jnp.cos(angles) - second_half * jnp.sin(angles),
            second_half * jnp.cos(angles) + first_half * jnp.sin(angles),
        ],
        axis=-1,
    )


def per_device(hidden_state, lengths, old_qkv, old_out, cache_keys, cache_values):
    seq_count = hidden_state.shape[0]
    local_joined = jnp.dot(hidden_state, old_qkv, preferred_element_type=jnp.float32).astype(
        jnp.bfloat16
    )
    joined_rows = lax.all_gather(local_joined, "tp", axis=1, tiled=True)
    q_width = HQ * HD
    k_width = KVH * HD
    group_size = HQ // KVH
    queries = rotate(
        joined_rows[:, :q_width].astype(jnp.float32).reshape(seq_count, HQ, HD), lengths
    ).astype(jnp.bfloat16)
    own_keys = rotate(
        joined_rows[:, q_width : q_width + k_width].astype(jnp.float32).reshape(seq_count, KVH, HD),
        lengths,
    ).astype(jnp.bfloat16)
    own_values = joined_rows[:, q_width + k_width :].reshape(seq_count, KVH, HD)
    inv_root = 1.0 / jnp.sqrt(jnp.float32(HD))
    cache_rows = cache_keys.shape[1]
    grouped = queries.reshape(seq_count, KVH, group_size, HD)
    key_blocks = cache_keys.reshape(seq_count, cache_rows, KVH, HD)
    value_blocks = cache_values.reshape(seq_count, cache_rows, KVH, HD)
    scores = (
        jnp.einsum("skgd,stkd->skgt", grouped, key_blocks, preferred_element_type=jnp.float32)
        * inv_root
    )
    positions = lax.axis_index("tp") * cache_rows + jnp.arange(cache_rows, dtype=jnp.int32)
    live_mask = (positions[None, :] < lengths[:, None])[:, None, None, :]
    scores = jnp.where(live_mask, scores, jnp.float32(-1e30))
    own_score = (
        jnp.sum(grouped.astype(jnp.float32) * own_keys.astype(jnp.float32)[:, :, None, :], axis=-1)
        * inv_root
    )
    local_top = jnp.maximum(jnp.max(scores, axis=-1), own_score)
    top_score = lax.pmax(local_top, "tp")
    weights = jnp.where(live_mask, jnp.exp(scores - top_score[..., None]), jnp.float32(0.0)).astype(
        jnp.bfloat16
    )
    numer_part = jnp.einsum(
        "skgt,stkd->skgd", weights, value_blocks, preferred_element_type=jnp.float32
    )
    denom_part = jnp.sum(weights.astype(jnp.float32), axis=-1)
    numerator, denominator = lax.psum((numer_part, denom_part), "tp")
    own_weight = lax.optimization_barrier(
        jnp.exp(own_score - top_score).astype(jnp.bfloat16)
    ).astype(jnp.float32)
    numerator = numerator + own_weight[..., None] * own_values.astype(jnp.float32)[:, :, None, :]
    denominator = denominator + own_weight
    attended = (numerator / denominator[..., None]).reshape(seq_count, q_width).astype(jnp.bfloat16)
    decoded = jnp.dot(attended, old_out, preferred_element_type=jnp.float32).astype(jnp.bfloat16)
    return decoded


def native_move(new_qkv, new_out):
    def move(block):
        piece = lax.all_to_all(block, "tp", split_axis=1, concat_axis=0, tiled=True)
        return lax.all_gather(piece, "rep", axis=0, tiled=True)

    return move(new_qkv), move(new_out)


def flip(index, bits, size):
    out = index
    bit = 1
    while bit < size:
        if (bits // bit) % 2:
            out = out + bit - 2 * bit * ((index // bit) % 2)
        bit *= 2
    return out


def step_kernel(
    planes, tps,
    hidden, cosine, sine, live, old_qkv, old_out, keys, values, new_qkv, new_out,
    decoded, qkv_full, out_full,
    a_send, a_recv, u_send, u_recv, d_send, d_recv, s_send, s_recv, own_sem, load_sem,
    j_send, j_recv, n_send, n_recv,
    w_qkv, w_out, k_held, v_held, joined, rotated, own_score, own_value, parts, attended,
):
    rep, tp = lax.axis_index("rep"), lax.axis_index("tp")
    plane, core = rep // 2, rep % 2
    rows = new_qkv.shape[0]
    blocks, fulls = (new_qkv, new_out), (qkv_full, out_full)
    widths = (qkv_full.shape[1], out_full.shape[1])
    up = (jnp.minimum(plane + 1, planes - 1) * 2 + core, tp)
    down = (jnp.maximum(plane - 1, 0) * 2 + core, tp)
    twin = (plane * 2 + 1 - core, tp)
    peers = [(rep, flip(tp, k, tps)) for k in range(1, tps)]
    can_up, can_down = plane < planes - 1, plane > 0

    barrier = pltpu.get_barrier_semaphore()
    for device in [twin] + peers:
        pl.semaphore_signal(barrier, inc=1, device_id=device, device_id_type=MESH)

    @pl.when(can_up)
    def _():
        pl.semaphore_signal(barrier, inc=1, device_id=up, device_id_type=MESH)

    @pl.when(can_down)
    def _():
        pl.semaphore_signal(barrier, inc=1, device_id=down, device_id_type=MESH)

    @pl.when(can_up & can_down)
    def _():
        pl.semaphore_wait(barrier, tps + 2)

    @pl.when(jnp.logical_not(can_up & can_down))
    def _():
        pl.semaphore_wait(barrier, tps + 1)

    def remote(source, target, send, recv, device):
        return pltpu.make_async_remote_copy(
            src_ref=source, dst_ref=target, send_sem=send, recv_sem=recv,
            device_id=device, device_id_type=MESH,
        )

    def rows_of(source_plane, source_core, k, w):
        start = ((source_plane * 2 + source_core) * tps + flip(tp, k, tps)) * rows
        return fulls[w].at[pl.ds(pl.multiple_of(start, rows), rows)]

    def column(w, t):
        return blocks[w].at[:, pl.ds(pl.multiple_of(t * widths[w], 128), widths[w])]

    def in_plane(k, w):
        return remote(
            column(w, flip(tp, k, tps)), rows_of(plane, core, 0, w),
            a_send.at[k, w], a_recv.at[k, w], peers[k - 1],
        )

    def piece(d, k, w):
        target = rows_of(plane - d, core, k, w)
        return target, (column(w, tp) if d == 0 and k == 0 else target)

    def to_up(d, k, w):
        target, source = piece(d, k, w)
        return remote(source, target, u_send.at[d, k, w], u_recv.at[d, k, w], up)

    def to_down(d, k, w):
        target, source = piece(-d, k, w)
        return remote(source, target, d_send.at[d, k, w], d_recv.at[d, k, w], down)

    def to_twin(d, k, w):
        target, source = piece(d, k, w)
        slot = d + planes - 1
        return remote(source, target, s_send.at[slot, k, w], s_recv.at[slot, k, w], twin)

    def own(k, w):
        @pl.when(can_up)
        def _():
            to_up(0, k, w).start()

        @pl.when(can_down)
        def _():
            to_down(0, k, w).start()

        to_twin(0, k, w).start()

    def relay(d):
        for k in range(tps):
            for w in range(2):

                @pl.when(plane >= d)
                def _():
                    target = rows_of(plane - d, core, k, w)
                    remote(
                        target, target, u_send.at[d - 1, k, w], u_recv.at[d - 1, k, w], up
                    ).wait_recv()

                    @pl.when(can_up)
                    def _():
                        to_up(d, k, w).start()

                    to_twin(d, k, w).start()

                @pl.when(plane + d < planes)
                def _():
                    target = rows_of(plane + d, core, k, w)
                    remote(
                        target, target, d_send.at[d - 1, k, w], d_recv.at[d - 1, k, w], down
                    ).wait_recv()

                    @pl.when(can_down)
                    def _():
                        to_down(d, k, w).start()

                    to_twin(-d, k, w).start()

    for k in range(1, tps):
        for w in range(2):
            in_plane(k, w).start()
    for w in range(2):
        own(0, w)
    locals_ = [
        pltpu.make_async_copy(column(w, tp), rows_of(plane, core, 0, w), own_sem.at[w])
        for w in range(2)
    ]
    loads = [
        pltpu.make_async_copy(source, target, load_sem.at[i])
        for i, (source, target) in enumerate(
            ((old_qkv, w_qkv), (keys, k_held), (values, v_held), (old_out, w_out))
        )
    ]
    for copy in locals_ + loads:
        copy.start()
    for k in range(1, tps):
        for w in range(2):
            target = rows_of(plane, core, k, w)
            remote(
                target, target, a_send.at[k, w], a_recv.at[k, w], peers[k - 1]
            ).wait_recv()
            own(k, w)

    seqs = hidden.shape[0]
    tile = 128
    loads[0].wait()

    @pl.loop(0, w_qkv.shape[1] // tile)
    def _(i):
        at = pl.ds(pl.multiple_of(i * tile, tile), tile)
        joined[tp, :, at] = jnp.dot(
            hidden[...], w_qkv[:, at], preferred_element_type=jnp.float32
        ).astype(joined.dtype)

    def send_joined(k):
        return remote(
            joined.at[tp], joined.at[tp], j_send.at[k], j_recv.at[k], peers[k - 1]
        )

    for k in range(1, tps):
        send_joined(k).start()

    relay(1)

    for k in range(1, tps):
        slot = joined.at[flip(tp, k, tps)]
        remote(slot, slot, j_send.at[k], j_recv.at[k], peers[k - 1]).wait_recv()
    for copy in loads[1:]:
        copy.wait()

    group = HQ // KVH
    per_slot = joined.shape[2] // HD
    inv_root = 1.0 / jnp.sqrt(jnp.float32(HD))

    def head(j):
        at = (j % per_slot) * HD
        return joined[j // per_slot, :, at : at + HD].astype(jnp.float32)

    def turn(v):
        swapped = jnp.concatenate([v[:, HD // 2 :], v[:, : HD // 2]], axis=1)
        return (v * cosine[...] + swapped * sine[...]).astype(jnp.bfloat16).astype(jnp.float32)

    rotated[...] = jnp.zeros_like(rotated)
    own_score[...] = jnp.zeros_like(own_score)
    own_value[...] = jnp.zeros_like(own_value)
    for kv in range(KVH):
        own_key = turn(head(HQ + kv))
        new_value = head(HQ + KVH + kv)
        for g in range(group):
            query = turn(head(kv * group + g))
            rotated[:, kv * PAD + g, :] = query
            score = jnp.sum(query * own_key, axis=1, keepdims=True) * inv_root
            own_score[:, kv * PAD + g, :] = jnp.broadcast_to(score, (seqs, HD))
            own_value[:, kv * PAD + g, :] = new_value

    @pl.loop(0, seqs)
    def _(s):
        is_live = live[pl.ds(s, 1), :] > 0.0
        for kv in range(KVH):
            at = slice(kv * HD, (kv + 1) * HD)
            lanes = slice(kv * PAD, (kv + 1) * PAD)
            query = rotated[s, lanes, :].astype(jnp.bfloat16)
            scores = lax.dot_general(
                query, k_held[s, :, at], (((1,), (1,)), ((), ())),
                preferred_element_type=jnp.float32,
            ) * inv_root
            scores = jnp.where(is_live, scores, jnp.float32(-1e30))
            top = jnp.max(scores, axis=1, keepdims=True)
            weights = jnp.where(is_live, jnp.exp(scores - top), 0.0).astype(jnp.bfloat16)
            total = jnp.sum(weights.astype(jnp.float32), axis=1, keepdims=True)
            parts[tp, 0, s, lanes, :] = jnp.dot(
                weights, v_held[s, :, at], preferred_element_type=jnp.float32
            )
            parts[tp, 1, s, lanes, :] = jnp.broadcast_to(top, (PAD, HD))
            parts[tp, 2, s, lanes, :] = jnp.broadcast_to(total, (PAD, HD))

    def send_parts(k):
        return remote(parts.at[tp], parts.at[tp], n_send.at[k], n_recv.at[k], peers[k - 1])

    for k in range(1, tps):
        send_parts(k).start()

    for d in range(2, planes - 1):
        relay(d)

    for k in range(1, tps):
        slot = parts.at[flip(tp, k, tps)]
        remote(slot, slot, n_send.at[k], n_recv.at[k], peers[k - 1]).wait_recv()

    @pl.loop(0, seqs)
    def _(s):
        mine = own_score[s]
        top = mine
        for t in range(tps):
            top = jnp.maximum(top, parts[t, 1, s])
        mine = jnp.exp(mine - top).astype(jnp.bfloat16).astype(jnp.float32)
        numerator, denominator = mine * own_value[s], mine
        for t in range(tps):
            scale = jnp.exp(parts[t, 1, s] - top)
            numerator = numerator + parts[t, 0, s] * scale
            denominator = denominator + parts[t, 2, s] * scale
        rotated[s] = numerator / denominator

    for j in range(HQ):
        row = (j // group) * PAD + j % group
        attended[:, j * HD : (j + 1) * HD] = rotated[:, row, :].astype(attended.dtype)

    @pl.loop(0, w_out.shape[1] // tile)
    def _(i):
        at = pl.ds(pl.multiple_of(i * tile, tile), tile)
        decoded[:, at] = jnp.dot(
            attended[...], w_out[:, at], preferred_element_type=jnp.float32
        ).astype(decoded.dtype)

    relay(planes - 1)

    for d in range(planes):
        for k in range(tps):
            for w in range(2):

                def from_twin(e):
                    target = rows_of(plane - e, 1 - core, k, w)
                    slot = e + planes - 1
                    return remote(
                        target, target, s_send.at[slot, k, w], s_recv.at[slot, k, w], twin
                    )

                @pl.when(plane >= d)
                def _():
                    from_twin(d).wait_recv()
                    to_twin(d, k, w).wait_send()

                    @pl.when(can_up)
                    def _():
                        to_up(d, k, w).wait_send()

                if d:

                    @pl.when(plane + d < planes)
                    def _():
                        from_twin(-d).wait_recv()
                        to_twin(-d, k, w).wait_send()

                @pl.when((plane + d < planes) & can_down)
                def _():
                    to_down(d, k, w).wait_send()

    for k in range(1, tps):
        for w in range(2):
            in_plane(k, w).wait_send()
        send_joined(k).wait_send()
        send_parts(k).wait_send()
    for copy in locals_:
        copy.wait()


def fused(mesh, hidden, lengths, old_qkv, old_out, keys, values, new_qkv, new_out):
    reps, tps = mesh.shape["rep"], mesh.shape["tp"]
    planes = reps // 2
    seqs, positions = keys.shape[:2]
    rows = new_qkv.shape[0]
    widths = (new_qkv.shape[1] // tps, new_out.shape[1] // tps)
    half = HD // 2
    frequency = ROPE_BASE ** (-2.0 * jnp.arange(half, dtype=jnp.float32) / (2 * half))
    angles = lengths.astype(jnp.float32)[:, None] * frequency
    cosine, sine = jnp.cos(angles), jnp.sin(angles)
    cosine = jnp.concatenate([cosine, cosine], axis=1)
    sine = jnp.concatenate([-sine, sine], axis=1)
    places = lax.axis_index("tp") * positions + jnp.arange(positions, dtype=jnp.int32)
    live = (places[None, :] < lengths[:, None]).astype(jnp.float32)

    sem = pltpu.SemaphoreType.DMA
    whole, anywhere = pl.BlockSpec(memory_space=pltpu.VMEM), pl.BlockSpec(memory_space=pl.ANY)
    in_hbm = pl.BlockSpec(memory_space=pltpu.HBM)
    f32, bf16 = jnp.float32, jnp.bfloat16
    padded = KVH * PAD
    landed = 2 * rows * reps * tps * sum(widths)
    scratch = [sem((tps, 2)), sem((tps, 2))]
    scratch += [sem((planes, tps, 2)) for _ in range(4)]
    scratch += [sem((2 * planes - 1, tps, 2)) for _ in range(2)]
    scratch += [sem((2,)), sem((4,))] + [sem((tps,)) for _ in range(4)]
    scratch += [pltpu.VMEM(x.shape, x.dtype) for x in (old_qkv, old_out, keys, values)]
    scratch += [
        pltpu.VMEM((tps, seqs, widths[0]), bf16),
        pltpu.VMEM((seqs, padded, HD), f32),
        pltpu.VMEM((seqs, padded, HD), f32),
        pltpu.VMEM((seqs, padded, HD), f32),
        pltpu.VMEM((tps, 3, seqs, padded, HD), f32),
        pltpu.VMEM((seqs, HQ * HD), bf16),
    ]
    return pl.pallas_call(
        functools.partial(step_kernel, planes, tps),
        out_shape=[jax.ShapeDtypeStruct((seqs, widths[1]), bf16)]
        + [pltpu.VMEM((rows * reps * tps, width), bf16) for width in widths],
        in_specs=[whole] * 4 + [in_hbm] * 6,
        out_specs=[whole] + [anywhere] * 2,
        scratch_shapes=scratch,
        compiler_params=pltpu.CompilerParams(
            collective_id=0, has_side_effects=True, vmem_limit_bytes=VMEM_BYTES - landed - SLACK
        ),
    )(hidden, cosine, sine, live, old_qkv, old_out, keys, values, new_qkv, new_out)


def solution(mesh):
    in_specs = (
        P("rep", None),
        P("rep"),
        P(None, "tp"),
        P(None, "tp"),
        P("rep", "tp", None),
        P("rep", "tp", None),
        P(("rep", "tp"), None),
        P(("rep", "tp"), None),
    )
    out_specs = (P("rep", "tp"), P(None, "tp"), P(None, "tp"))

    def step(*args):
        reps, tps = mesh.shape["rep"], mesh.shape["tp"]
        widths = [x.shape[1] // tps for x in args[6:]]
        tiled = args[6].shape[0] % 16 == 0 and all(width % 128 == 0 for width in widths)
        if reps % 4 or not tiled:
            return (per_device(*args[:6]), *native_move(*args[6:]))
        return tuple(fused(mesh, *args))

    return jax.shard_map(
        step, mesh=mesh, in_specs=in_specs, out_specs=out_specs, check_vma=False
    )
```

```python
import functools

import jax
import jax.numpy as jnp
import numpy as np
from jax import lax
from jax.experimental import pallas as pl
from jax.experimental.pallas import tpu as pltpu
from jax.sharding import PartitionSpec as P

HQ = 28
KVH = 4
HD = 128
PAD = 8
CUTS = 8
VMEM_BYTES = 67043328
SLACK = 600000
MESH = pl.DeviceIdType.MESH


ROPE_BASE = 1000000.0


def rotate(vectors, positions):
    half_dim = vectors.shape[-1] // 2
    frequency = ROPE_BASE ** (-2.0 * jnp.arange(half_dim, dtype=jnp.float32) / (2 * half_dim))
    angles = positions.astype(jnp.float32)[:, None, None] * frequency
    first_half = vectors[..., :half_dim]
    second_half = vectors[..., half_dim:]
    return jnp.concatenate(
        [
            first_half * jnp.cos(angles) - second_half * jnp.sin(angles),
            second_half * jnp.cos(angles) + first_half * jnp.sin(angles),
        ],
        axis=-1,
    )


def per_device(hidden_state, lengths, old_qkv, old_out, cache_keys, cache_values):
    seq_count = hidden_state.shape[0]
    local_joined = jnp.dot(hidden_state, old_qkv, preferred_element_type=jnp.float32).astype(
        jnp.bfloat16
    )
    joined_rows = lax.all_gather(local_joined, "tp", axis=1, tiled=True)
    q_width = HQ * HD
    k_width = KVH * HD
    group_size = HQ // KVH
    queries = rotate(
        joined_rows[:, :q_width].astype(jnp.float32).reshape(seq_count, HQ, HD), lengths
    ).astype(jnp.bfloat16)
    own_keys = rotate(
        joined_rows[:, q_width : q_width + k_width].astype(jnp.float32).reshape(seq_count, KVH, HD),
        lengths,
    ).astype(jnp.bfloat16)
    own_values = joined_rows[:, q_width + k_width :].reshape(seq_count, KVH, HD)
    inv_root = 1.0 / jnp.sqrt(jnp.float32(HD))
    cache_rows = cache_keys.shape[1]
    grouped = queries.reshape(seq_count, KVH, group_size, HD)
    key_blocks = cache_keys.reshape(seq_count, cache_rows, KVH, HD)
    value_blocks = cache_values.reshape(seq_count, cache_rows, KVH, HD)
    scores = (
        jnp.einsum("skgd,stkd->skgt", grouped, key_blocks, preferred_element_type=jnp.float32)
        * inv_root
    )
    positions = lax.axis_index("tp") * cache_rows + jnp.arange(cache_rows, dtype=jnp.int32)
    live_mask = (positions[None, :] < lengths[:, None])[:, None, None, :]
    scores = jnp.where(live_mask, scores, jnp.float32(-1e30))
    own_score = (
        jnp.sum(grouped.astype(jnp.float32) * own_keys.astype(jnp.float32)[:, :, None, :], axis=-1)
        * inv_root
    )
    local_top = jnp.maximum(jnp.max(scores, axis=-1), own_score)
    top_score = lax.pmax(local_top, "tp")
    weights = jnp.where(live_mask, jnp.exp(scores - top_score[..., None]), jnp.float32(0.0)).astype(
        jnp.bfloat16
    )
    numer_part = jnp.einsum(
        "skgt,stkd->skgd", weights, value_blocks, preferred_element_type=jnp.float32
    )
    denom_part = jnp.sum(weights.astype(jnp.float32), axis=-1)
    numerator, denominator = lax.psum((numer_part, denom_part), "tp")
    own_weight = lax.optimization_barrier(
        jnp.exp(own_score - top_score).astype(jnp.bfloat16)
    ).astype(jnp.float32)
    numerator = numerator + own_weight[..., None] * own_values.astype(jnp.float32)[:, :, None, :]
    denominator = denominator + own_weight
    attended = (numerator / denominator[..., None]).reshape(seq_count, q_width).astype(jnp.bfloat16)
    decoded = jnp.dot(attended, old_out, preferred_element_type=jnp.float32).astype(jnp.bfloat16)
    return decoded


def native_move(new_qkv, new_out):
    def move(block):
        piece = lax.all_to_all(block, "tp", split_axis=1, concat_axis=0, tiled=True)
        return lax.all_gather(piece, "rep", axis=0, tiled=True)

    return move(new_qkv), move(new_out)


def flip(index, bits, size):
    out = index
    bit = 1
    while bit < size:
        if (bits // bit) % 2:
            out = out + bit - 2 * bit * ((index // bit) % 2)
        bit *= 2
    return out


def step_kernel(
    planes, tps,
    hidden, lengths, frequency, old_qkv, old_out, keys, values, new_qkv, new_out,
    decoded, qkv_full, out_full,
    a_send, a_recv, u_send, u_recv, d_send, d_recv, s_send, s_recv, own_sem, load_sem,
    j_send, j_recv, n_send, n_recv,
    w_qkv, w_out, k_held, v_held, joined, rotated, own_score, own_value, parts, attended,
    cosine, sine,
):
    rep, tp = lax.axis_index("rep"), lax.axis_index("tp")
    plane, core = rep // 2, rep % 2
    rows = new_qkv.shape[0]
    blocks, fulls = (new_qkv, new_out), (qkv_full, out_full)
    widths = (qkv_full.shape[1], out_full.shape[1])
    up = (jnp.minimum(plane + 1, planes - 1) * 2 + core, tp)
    down = (jnp.maximum(plane - 1, 0) * 2 + core, tp)
    twin = (plane * 2 + 1 - core, tp)
    peers = [(rep, flip(tp, k, tps)) for k in range(1, tps)]
    can_up, can_down = plane < planes - 1, plane > 0

    barrier = pltpu.get_barrier_semaphore()
    for device in [twin] + peers:
        pl.semaphore_signal(barrier, inc=1, device_id=device, device_id_type=MESH)

    @pl.when(can_up)
    def _():
        pl.semaphore_signal(barrier, inc=1, device_id=up, device_id_type=MESH)

    @pl.when(can_down)
    def _():
        pl.semaphore_signal(barrier, inc=1, device_id=down, device_id_type=MESH)

    @pl.when(can_up & can_down)
    def _():
        pl.semaphore_wait(barrier, tps + 2)

    @pl.when(jnp.logical_not(can_up & can_down))
    def _():
        pl.semaphore_wait(barrier, tps + 1)

    def remote(source, target, send, recv, device):
        return pltpu.make_async_remote_copy(
            src_ref=source, dst_ref=target, send_sem=send, recv_sem=recv,
            device_id=device, device_id_type=MESH,
        )

    def rows_of(source_plane, source_core, k, w):
        start = ((source_plane * 2 + source_core) * tps + flip(tp, k, tps)) * rows
        return fulls[w].at[pl.ds(pl.multiple_of(start, rows), rows)]

    def column(w, t):
        return blocks[w].at[:, pl.ds(pl.multiple_of(t * widths[w], 128), widths[w])]

    def in_plane(k, w):
        return remote(
            column(w, flip(tp, k, tps)), rows_of(plane, core, 0, w),
            a_send.at[k, w], a_recv.at[k, w], peers[k - 1],
        )

    def piece(d, k, w):
        target = rows_of(plane - d, core, k, w)
        return target, (column(w, tp) if d == 0 and k == 0 else target)

    def to_up(d, k, w):
        target, source = piece(d, k, w)
        return remote(source, target, u_send.at[d, k, w], u_recv.at[d, k, w], up)

    def to_down(d, k, w):
        target, source = piece(-d, k, w)
        return remote(source, target, d_send.at[d, k, w], d_recv.at[d, k, w], down)

    def to_twin(d, k, w):
        target, source = piece(d, k, w)
        slot = d + planes - 1
        return remote(source, target, s_send.at[slot, k, w], s_recv.at[slot, k, w], twin)

    def own(k, w):
        @pl.when(can_up)
        def _():
            to_up(0, k, w).start()

        @pl.when(can_down)
        def _():
            to_down(0, k, w).start()

        to_twin(0, k, w).start()

    def relay(d):
        for k in range(tps):
            for w in range(2):

                @pl.when(plane >= d)
                def _():
                    target = rows_of(plane - d, core, k, w)
                    remote(
                        target, target, u_send.at[d - 1, k, w], u_recv.at[d - 1, k, w], up
                    ).wait_recv()

                    @pl.when(can_up)
                    def _():
                        to_up(d, k, w).start()

                    to_twin(d, k, w).start()

                @pl.when(plane + d < planes)
                def _():
                    target = rows_of(plane + d, core, k, w)
                    remote(
                        target, target, d_send.at[d - 1, k, w], d_recv.at[d - 1, k, w], down
                    ).wait_recv()

                    @pl.when(can_down)
                    def _():
                        to_down(d, k, w).start()

                    to_twin(-d, k, w).start()

    for k in range(1, tps):
        for w in range(2):
            in_plane(k, w).start()
    for w in range(2):
        own(0, w)
    locals_ = [
        pltpu.make_async_copy(column(w, tp), rows_of(plane, core, 0, w), own_sem.at[w])
        for w in range(2)
    ]
    loads = [
        pltpu.make_async_copy(source, target, load_sem.at[i])
        for i, (source, target) in enumerate(
            ((old_qkv, w_qkv), (keys, k_held), (values, v_held), (old_out, w_out))
        )
    ]
    for copy in locals_ + loads:
        copy.start()
    for k in range(1, tps):
        for w in range(2):
            target = rows_of(plane, core, k, w)
            remote(
                target, target, a_send.at[k, w], a_recv.at[k, w], peers[k - 1]
            ).wait_recv()
            own(k, w)

    seqs = hidden.shape[0]
    lane = lax.broadcasted_iota(jnp.int32, (1, HD), 1)
    for s in range(seqs):
        angles = lengths[s].astype(jnp.float32) * frequency[...]
        cosine[s : s + 1, :] = jnp.cos(angles)
        sine[s : s + 1, :] = jnp.where(lane < HD // 2, -jnp.sin(angles), jnp.sin(angles))
    tile = 128
    loads[0].wait()

    @pl.loop(0, w_qkv.shape[1] // tile)
    def _(i):
        at = pl.ds(pl.multiple_of(i * tile, tile), tile)
        joined[tp, :, at] = jnp.dot(
            hidden[...], w_qkv[:, at], preferred_element_type=jnp.float32
        ).astype(joined.dtype)

    def send_joined(k):
        return remote(
            joined.at[tp], joined.at[tp], j_send.at[k], j_recv.at[k], peers[k - 1]
        )

    for k in range(1, tps):
        send_joined(k).start()

    relay(1)

    for k in range(1, tps):
        slot = joined.at[flip(tp, k, tps)]
        remote(slot, slot, j_send.at[k], j_recv.at[k], peers[k - 1]).wait_recv()
    for copy in loads[1:]:
        copy.wait()

    group = HQ // KVH
    positions = k_held.shape[1]
    per_slot = joined.shape[2] // HD
    inv_root = 1.0 / jnp.sqrt(jnp.float32(HD))

    def head(j):
        at = (j % per_slot) * HD
        return joined[j // per_slot, :, at : at + HD].astype(jnp.float32)

    def turn(v):
        swapped = jnp.concatenate([v[:, HD // 2 :], v[:, : HD // 2]], axis=1)
        return (v * cosine[...] + swapped * sine[...]).astype(jnp.bfloat16).astype(jnp.float32)

    rotated[...] = jnp.zeros_like(rotated)
    own_score[...] = jnp.zeros_like(own_score)
    own_value[...] = jnp.zeros_like(own_value)
    for kv in range(KVH):
        own_key = turn(head(HQ + kv))
        new_value = head(HQ + KVH + kv)
        for g in range(group):
            query = turn(head(kv * group + g))
            rotated[:, kv * PAD + g, :] = query
            score = jnp.sum(query * own_key, axis=1, keepdims=True) * inv_root
            own_score[:, kv * PAD + g, :] = jnp.broadcast_to(score, (seqs, HD))
            own_value[:, kv * PAD + g, :] = new_value

    @pl.loop(0, seqs)
    def _(s):
        place = lax.broadcasted_iota(jnp.int32, (1, positions), 1) + tp * positions
        is_live = place < lengths[s]
        for kv in range(KVH):
            at = slice(kv * HD, (kv + 1) * HD)
            lanes = slice(kv * PAD, (kv + 1) * PAD)
            query = rotated[s, lanes, :].astype(jnp.bfloat16)
            scores = lax.dot_general(
                query, k_held[s, :, at], (((1,), (1,)), ((), ())),
                preferred_element_type=jnp.float32,
            ) * inv_root
            scores = jnp.where(is_live, scores, jnp.float32(-1e30))
            top = jnp.max(scores, axis=1, keepdims=True)
            weights = jnp.where(is_live, jnp.exp(scores - top), 0.0).astype(jnp.bfloat16)
            total = jnp.sum(weights.astype(jnp.float32), axis=1, keepdims=True)
            parts[tp, 0, s, lanes, :] = jnp.dot(
                weights, v_held[s, :, at], preferred_element_type=jnp.float32
            )
            parts[tp, 1, s, lanes, :] = jnp.broadcast_to(top, (PAD, HD))
            parts[tp, 2, s, lanes, :] = jnp.broadcast_to(total, (PAD, HD))

    def send_parts(k):
        return remote(parts.at[tp], parts.at[tp], n_send.at[k], n_recv.at[k], peers[k - 1])

    for k in range(1, tps):
        send_parts(k).start()

    for d in range(2, planes - 1):
        relay(d)

    for k in range(1, tps):
        slot = parts.at[flip(tp, k, tps)]
        remote(slot, slot, n_send.at[k], n_recv.at[k], peers[k - 1]).wait_recv()

    @pl.loop(0, seqs)
    def _(s):
        mine = own_score[s]
        top = mine
        for t in range(tps):
            top = jnp.maximum(top, parts[t, 1, s])
        mine = jnp.exp(mine - top).astype(jnp.bfloat16).astype(jnp.float32)
        numerator, denominator = mine * own_value[s], mine
        for t in range(tps):
            scale = jnp.exp(parts[t, 1, s] - top)
            numerator = numerator + parts[t, 0, s] * scale
            denominator = denominator + parts[t, 2, s] * scale
        rotated[s] = numerator / denominator

    for j in range(HQ):
        row = (j // group) * PAD + j % group
        attended[:, j * HD : (j + 1) * HD] = rotated[:, row, :].astype(attended.dtype)

    @pl.loop(0, w_out.shape[1] // tile)
    def _(i):
        at = pl.ds(pl.multiple_of(i * tile, tile), tile)
        decoded[:, at] = jnp.dot(
            attended[...], w_out[:, at], preferred_element_type=jnp.float32
        ).astype(decoded.dtype)

    relay(planes - 1)

    for d in range(planes):
        for k in range(tps):
            for w in range(2):

                def from_twin(e):
                    target = rows_of(plane - e, 1 - core, k, w)
                    slot = e + planes - 1
                    return remote(
                        target, target, s_send.at[slot, k, w], s_recv.at[slot, k, w], twin
                    )

                @pl.when(plane >= d)
                def _():
                    from_twin(d).wait_recv()
                    to_twin(d, k, w).wait_send()

                    @pl.when(can_up)
                    def _():
                        to_up(d, k, w).wait_send()

                if d:

                    @pl.when(plane + d < planes)
                    def _():
                        from_twin(-d).wait_recv()
                        to_twin(-d, k, w).wait_send()

                @pl.when((plane + d < planes) & can_down)
                def _():
                    to_down(d, k, w).wait_send()

    for k in range(1, tps):
        for w in range(2):
            in_plane(k, w).wait_send()
        send_joined(k).wait_send()
        send_parts(k).wait_send()
    for copy in locals_:
        copy.wait()


def flush_kernel(decoded, qkv, out, decoded_to, qkv_to, out_to, sems):
    copies = [pltpu.make_async_copy(decoded, decoded_to, sems.at[0])]
    for source, target in ((qkv, qkv_to), (out, out_to)):
        rows = source.shape[0] // CUTS
        for i in range(CUTS):
            at = pl.ds(i * rows, rows)
            copies.append(
                pltpu.make_async_copy(source.at[at], target.at[at], sems.at[len(copies)])
            )
    for copy in copies:
        copy.start()
    for copy in copies:
        copy.wait()


def flush(*arrays):
    return pl.pallas_call(
        flush_kernel,
        out_shape=[jax.ShapeDtypeStruct(x.shape, x.dtype) for x in arrays],
        in_specs=[pl.BlockSpec(memory_space=pltpu.VMEM)] * 3,
        out_specs=[pl.BlockSpec(memory_space=pltpu.HBM)] * 3,
        scratch_shapes=[pltpu.SemaphoreType.DMA((2 * CUTS + 1,))],
        compiler_params=pltpu.CompilerParams(vmem_limit_bytes=2**20),
    )(*arrays)


def fused(mesh, hidden, lengths, old_qkv, old_out, keys, values, new_qkv, new_out):
    reps, tps = mesh.shape["rep"], mesh.shape["tp"]
    planes = reps // 2
    seqs = keys.shape[0]
    rows = new_qkv.shape[0]
    widths = (new_qkv.shape[1] // tps, new_out.shape[1] // tps)
    half = HD // 2
    frequency = ROPE_BASE ** (-2.0 * np.arange(half) / (2 * half))
    frequency = jnp.asarray(np.concatenate([frequency, frequency])[None], jnp.float32)

    sem = pltpu.SemaphoreType.DMA
    whole, anywhere = pl.BlockSpec(memory_space=pltpu.VMEM), pl.BlockSpec(memory_space=pl.ANY)
    in_hbm = pl.BlockSpec(memory_space=pltpu.HBM)
    f32, bf16 = jnp.float32, jnp.bfloat16
    padded = KVH * PAD
    landed = 2 * rows * reps * tps * sum(widths)
    scratch = [sem((tps, 2)), sem((tps, 2))]
    scratch += [sem((planes, tps, 2)) for _ in range(4)]
    scratch += [sem((2 * planes - 1, tps, 2)) for _ in range(2)]
    scratch += [sem((2,)), sem((4,))] + [sem((tps,)) for _ in range(4)]
    scratch += [pltpu.VMEM(x.shape, x.dtype) for x in (old_qkv, old_out, keys, values)]
    scratch += [
        pltpu.VMEM((tps, seqs, widths[0]), bf16),
        pltpu.VMEM((seqs, padded, HD), f32),
        pltpu.VMEM((seqs, padded, HD), f32),
        pltpu.VMEM((seqs, padded, HD), f32),
        pltpu.VMEM((tps, 3, seqs, padded, HD), f32),
        pltpu.VMEM((seqs, HQ * HD), bf16),
        pltpu.VMEM((seqs, HD), f32),
        pltpu.VMEM((seqs, HD), f32),
    ]
    return pl.pallas_call(
        functools.partial(step_kernel, planes, tps),
        out_shape=[pltpu.VMEM((seqs, widths[1]), bf16)]
        + [pltpu.VMEM((rows * reps * tps, width), bf16) for width in widths],
        in_specs=[whole, pl.BlockSpec(memory_space=pltpu.SMEM), whole] + [in_hbm] * 6,
        out_specs=[whole] + [anywhere] * 2,
        scratch_shapes=scratch,
        compiler_params=pltpu.CompilerParams(
            collective_id=0, has_side_effects=True, vmem_limit_bytes=VMEM_BYTES - landed - SLACK
        ),
    )(hidden, lengths, frequency, old_qkv, old_out, keys, values, new_qkv, new_out)


def solution(mesh):
    in_specs = (
        P("rep", None),
        P("rep"),
        P(None, "tp"),
        P(None, "tp"),
        P("rep", "tp", None),
        P("rep", "tp", None),
        P(("rep", "tp"), None),
        P(("rep", "tp"), None),
    )
    out_specs = (P("rep", "tp"), P(None, "tp"), P(None, "tp"))

    def step(*args):
        reps, tps = mesh.shape["rep"], mesh.shape["tp"]
        widths = [x.shape[1] // tps for x in args[6:]]
        tiled = args[6].shape[0] % 16 == 0 and all(width % 128 == 0 for width in widths)
        if reps % 4 or not tiled:
            return (per_device(*args[:6]), *native_move(*args[6:]))
        return tuple(flush(*fused(mesh, *args)))

    return jax.shard_map(
        step, mesh=mesh, in_specs=in_specs, out_specs=out_specs, check_vma=False
    )
```
